32 devices in a mesh: ep: 4 (over y, core), fsdp: 8 (over z, x).
Axes of the slice: x: 2, y: 2, z: 4, core: 2. Of those that a mesh axis runs over, the one named last changes fastest.
Arguments:
- master_down: float32 [16, 6400, 4096], P('ep', None, 'fsdp'), may hold values from -0.109375 to 0.109375
- second_down: bfloat16 [16, 6400, 4096], P('ep', None, 'fsdp'), may hold values from -0.0390625 to 0.0390625
- router_weight: float32 [4096, 16], P('fsdp', 'ep'), may hold values from -0.09375 to 0.09375
- router_gain: float32 [4096], P('fsdp'), may hold values from 0.25 to 1.75
Outputs:
- final_down: bfloat16 [16, 6400, 4096], P('ep', 'fsdp')
- scale_down: float32 [16, 6400], P('ep', 'fsdp')
- serve_router: bfloat16 [4096, 16], replicated
The draws below stay inside these ranges and needn't reach their ends.
All inputs are finite; a program needn't handle non-finite values.
Results may differ from the reference program's by a relative error of at most 0.001.
Values may be sent and summed in bfloat16 or wider, within the bound.
No kernel may reach another device: no remote copies, remote signals or barrier semaphores. Data moves between devices by JAX's collectives and lax.ppermute only.
A program may use at most 256 MiB of HBM per device.

```python
import jax
import jax.numpy as jnp
from jax import lax

EXPERTS = 16
D_MODEL = 4096
D_EXPERT = 6400


def raised(result, own_key, source, target, shards_of, factor):
    owner, partner = [(jnp.arange(result.shape[dim]) // (result.shape[dim] // shards_of)).reshape([-1 if axis == dim else 1 for axis in range(result.ndim)]) for dim in (source, target)]
    chosen = jax.random.permutation(own_key, shards_of)[partner]
    strong = (owner == chosen) | (owner == (partner + shards_of // 2) % shards_of)
    return jnp.where(strong, factor * result, result)


def steps_of(own_key, shape, shards, smallest, top_value):
    factor_of, own = 1.0, jax.random.fold_in(own_key, 6)
    for position, blocks in shards:
        draws = jnp.exp(jax.random.uniform(jax.random.fold_in(own, position), (blocks,), jnp.float32, smallest / len(shards), top_value / len(shards)))
        factor_of = factor_of * jnp.repeat(draws, shape[position] // blocks).reshape([-1 if axis == position else 1 for axis in range(len(shape))])
    return factor_of


def noise(rng, dims, width, limit, cuts=(), kind=jnp.bfloat16):
    drawn = width * jax.random.normal(rng, dims, jnp.float32)
    if cuts:
        drawn = drawn * steps_of(rng, dims, cuts, -0.22, 0.18)
    return jnp.clip(drawn, -limit, limit).astype(kind)


def heavy_noise(stream_key, dims, width, limit, cuts, heavy, kind=jnp.bfloat16):
    entries = width * jax.random.normal(stream_key, dims, jnp.float32)
    if cuts:
        entries = entries * steps_of(stream_key, dims, cuts, -0.22, 0.18)
    return jnp.clip(raised(entries, jax.random.fold_in(stream_key, 3), *heavy), -limit, limit).astype(kind)


def setup_inputs(seed: int = 0) -> dict:
    arg_keys = jax.random.split(jax.random.key(seed), 5)
    return {
        "master_down": heavy_noise(arg_keys[0], (EXPERTS, D_EXPERT, D_MODEL), D_EXPERT ** -0.5, 0.109375, ((0, 4), (2, 8)), (2, 1, 8, 2.0), jnp.float32),
        "second_down": noise(arg_keys[1], (EXPERTS, D_EXPERT, D_MODEL), (D_EXPERT * 4) ** -0.5, 0.0390625, ((0, 4), (2, 8))),
        "router_weight": noise(arg_keys[2], (D_MODEL, EXPERTS), D_MODEL ** -0.5, 0.09375, ((0, 8), (1, 4)), jnp.float32),
        "router_gain": jnp.clip(1.0 + 0.15 * jax.random.normal(arg_keys[3], (D_MODEL,), jnp.float32), 0.25, 1.75),
    }


def reference(master_down, second_down, router_weight, router_gain):
    merged_down = master_down + second_down.astype(jnp.float32)
    scale_down = jnp.sqrt(lax.optimization_barrier(jnp.sum(merged_down * merged_down, axis=2)))
    final_down = (merged_down / jnp.expand_dims(scale_down, 2)).astype(jnp.bfloat16)
    serve_router = (router_weight * router_gain[:, None]).astype(jnp.bfloat16)
    return (final_down, scale_down, serve_router)
```

```python
import jax
import jax.numpy as jnp
from jax import lax
from jax.experimental import pallas as pl
from jax.experimental.pallas import tpu as pltpu
from jax.sharding import PartitionSpec as P


def place(held, pieces, expert, experts):
    shards, rows, cols = pieces.shape

    def body(*refs):
        refs[-1][...] = refs[-2][...]

    piece_spec = pl.BlockSpec((None, rows, cols), lambda s: (s, 0, 0))
    return pl.pallas_call(
        body,
        grid=(shards,),
        in_specs=([] if held is None else [pl.BlockSpec(memory_space=pl.ANY)]) + [piece_spec],
        out_specs=pl.BlockSpec((None, rows, cols), lambda s: (expert, 0, s)),
        out_shape=jax.ShapeDtypeStruct((experts, rows, shards * cols), pieces.dtype),
        input_output_aliases={} if held is None else {0: 0},
        cost_estimate=pl.CostEstimate(flops=50 * pieces.size, transcendentals=0, bytes_accessed=4 * pieces.size),
        name="place",
    )(*([] if held is None else [held]), pieces)


def shards(master_down, second_down, router_weight, router_gain):
    experts, width, cols = master_down.shape
    count = lax.axis_size("fsdp")
    rows = width // count

    part_router = (router_weight * router_gain[:, None]).astype(jnp.bfloat16)
    all_router = lax.all_gather(part_router.T, ("ep", "fsdp"), axis=0, tiled=False)

    merged_down = master_down + second_down.astype(jnp.float32)
    part_total = jnp.sum(merged_down * merged_down, axis=2)
    total_down = jnp.sum(lax.all_gather(part_total, "fsdp", axis=0, tiled=False), axis=0)
    scale_down, all_router = lax.optimization_barrier((jnp.sqrt(total_down), all_router))

    scaled = []
    for expert in range(experts):
        if scaled:
            master_down, second_down, scaled[-1] = lax.optimization_barrier((master_down, second_down, scaled[-1]))
        merged = master_down[expert] + second_down[expert].astype(jnp.float32)
        scaled.append((merged / scale_down[expert][:, None]).astype(jnp.bfloat16))
    received = [lax.all_to_all(part, "fsdp", split_axis=0, concat_axis=0, tiled=True) for part in scaled]
    final_down = None
    for expert in range(experts):
        final_down = place(final_down, received[expert].reshape(count, rows, cols), expert, experts)

    groups = all_router.shape[0] // count
    serve_router = all_router.reshape(groups, count, *part_router.T.shape).transpose(1, 3, 0, 2)
    serve_router = serve_router.reshape(count * part_router.shape[0], groups * part_router.shape[1])
    own_scale = lax.dynamic_slice_in_dim(scale_down, lax.axis_index("fsdp") * rows, rows, axis=1)
    return (final_down, own_scale, serve_router)


def solution(mesh):
    return jax.shard_map(
        shards,
        mesh=mesh,
        in_specs=(P("ep", None, "fsdp"), P("ep", None, "fsdp"), P("fsdp", "ep"), P("fsdp")),
        out_specs=(P("ep", "fsdp", None), P("ep", "fsdp"), P()),
        check_vma=False,
    )
```

```python
import jax
import jax.numpy as jnp
from jax import lax
from jax.experimental import pallas as pl
from jax.experimental.pallas import tpu as pltpu
from jax.sharding import PartitionSpec as P


def place(held, pieces, expert, experts):
    shards, rows, cols = pieces.shape

    def body(*refs):
        refs[-1][...] = refs[-2][...]

    block = rows // 2 if rows % 32 == 0 else rows
    piece_spec = pl.BlockSpec((None, block, cols), lambda s, r: (s, r, 0))
    return pl.pallas_call(
        body,
        grid=(shards, rows // block),
        in_specs=([] if held is None else [pl.BlockSpec(memory_space=pl.ANY)]) + [piece_spec],
        out_specs=pl.BlockSpec((None, block, cols), lambda s, r: (expert, r, s)),
        out_shape=jax.ShapeDtypeStruct((experts, rows, shards * cols), pieces.dtype),
        input_output_aliases={} if held is None else {0: 0},
        cost_estimate=pl.CostEstimate(flops=50 * pieces.size, transcendentals=0, bytes_accessed=4 * pieces.size),
        name="place",
    )(*([] if held is None else [held]), pieces)


def shards(master_down, second_down, router_weight, router_gain):
    experts, width, cols = master_down.shape
    count = lax.axis_size("fsdp")
    rows = width // count

    merged_down = master_down + second_down.astype(jnp.float32)
    part_total = jnp.sum(merged_down * merged_down, axis=2).reshape(experts, count, rows).transpose(1, 0, 2)
    totals = lax.all_to_all(part_total, "fsdp", split_axis=0, concat_axis=0, tiled=True)
    own_scale = jnp.sqrt(jnp.sum(totals, axis=0))
    copies = jnp.broadcast_to(own_scale[None], (count, *own_scale.shape))
    scale_down = lax.all_to_all(copies, "fsdp", split_axis=0, concat_axis=0, tiled=True)

    part_router = (router_weight * router_gain[:, None]).astype(jnp.bfloat16).T
    scaled = []
    for expert in range(experts):
        if scaled:
            master_down, second_down, scaled[-1] = lax.optimization_barrier((master_down, second_down, scaled[-1]))
        merged = master_down[expert] + second_down[expert].astype(jnp.float32)
        scaled.append((merged / scale_down[:, expert].reshape(width, 1)).astype(jnp.bfloat16))
        if expert == 1:
            part_router, scaled[1] = lax.optimization_barrier((part_router, scaled[1]))
            part_router = lax.all_gather(part_router, "ep", axis=0, tiled=True)
    part_router, scaled[-1] = lax.optimization_barrier((part_router, scaled[-1]))
    serve_router = lax.all_gather(part_router, "fsdp", axis=1, tiled=True)
    serve_router, scaled[-1] = lax.optimization_barrier((serve_router, scaled[-1]))
    serve_router = serve_router.T
    received = [lax.all_to_all(part, "fsdp", split_axis=0, concat_axis=0, tiled=True) for part in scaled]
    final_down = None
    for expert in range(experts):
        final_down = place(final_down, received[expert].reshape(count, rows, cols), expert, experts)
    return (final_down, own_scale, serve_router)


def solution(mesh):
    return jax.shard_map(
        shards,
        mesh=mesh,
        in_specs=(P("ep", None, "fsdp"), P("ep", None, "fsdp"), P("fsdp", "ep"), P("fsdp")),
        out_specs=(P("ep", "fsdp", None), P("ep", "fsdp"), P()),
        check_vma=False,
    )
```
